8 devices in a mesh: tp: 2 (over z, y), dp: 4 (over x, core).
Axes of the slice: x: 2, y: 2, z: 1, core: 2. Of those that a mesh axis runs over, the one named last changes fastest.
Arguments:
- tokens: int32 [4, 1024], P('dp')
- labels: int32 [4, 1024], P('dp')
- embed: float32 [50304, 256], P('tp')
- ln_scales: float32 [2, 256], replicated
- w_q: float32 [256, 256], P(None, 'tp')
- w_kv: float32 [2, 256, 32], replicated
- w_o: float32 [256, 256], P('tp')
- w_gu: float32 [2, 256, 1024], P(None, None, 'tp')
- w_down: float32 [1024, 256], P('tp')
- m_embed: float32 [50304, 256], P('tp')
- m_ln_scales: float32 [2, 256], replicated
- m_w_q: float32 [256, 256], P(None, 'tp')
- m_w_kv: float32 [2, 256, 32], replicated
- m_w_o: float32 [256, 256], P('tp')
- m_w_gu: float32 [2, 256, 1024], P(None, None, 'tp')
- m_w_down: float32 [1024, 256], P('tp')
- v_embed: float32 [50304, 256], P('tp')
- v_ln_scales: float32 [2, 256], replicated
- v_w_q: float32 [256, 256], P(None, 'tp')
- v_w_kv: float32 [2, 256, 32], replicated
- v_w_o: float32 [256, 256], P('tp')
- v_w_gu: float32 [2, 256, 1024], P(None, None, 'tp')
- v_w_down: float32 [1024, 256], P('tp')
Outputs:
- output 1: float32 [50304, 256], P('tp')
- output 2: float32 [2, 256], replicated
- output 3: float32 [256, 256], P(None, 'tp')
- output 4: float32 [2, 256, 32], replicated
- output 5: float32 [256, 256], P('tp')
- output 6: float32 [2, 256, 1024], P(None, None, 'tp')
- output 7: float32 [1024, 256], P('tp')
- output 8: float32 [50304, 256], P('tp')
- output 9: float32 [2, 256], replicated
- output 10: float32 [256, 256], P(None, 'tp')
- output 11: float32 [2, 256, 32], replicated
- output 12: float32 [256, 256], P('tp')
- output 13: float32 [2, 256, 1024], P(None, None, 'tp')
- output 14: float32 [1024, 256], P('tp')
- output 15: float32 [50304, 256], P('tp')
- output 16: float32 [2, 256], replicated
- output 17: float32 [256, 256], P(None, 'tp')
- output 18: float32 [2, 256, 32], replicated
- output 19: float32 [256, 256], P('tp')
- output 20: float32 [2, 256, 1024], P(None, None, 'tp')
- output 21: float32 [1024, 256], P('tp')
- output 22: float32 [], replicated
All inputs are finite; a program needn't handle non-finite values.
Results may differ from the reference program's by a relative error of at most 0.00956925.
Values sent between devices are 32-bit elements.
A program may use at most 1 GiB of HBM per device.

```python
import jax
import jax.numpy as jnp
from jax import lax

BATCH_ALL = 4
SEQ_LEN = 1024
D_MODEL = 256
N_HEADS = 8
HEAD_DIM = 32
FF_DIM = 1024
VOCAB_SIZE = 50304

LN_EPS = 1e-5
LOGIT_ZLOSS = 1e-4
LEARN_RATE = 1e-2
BETA_ONE = 0.9
BETA_TWO = 0.95
ADAM_EPS = 1e-8
ROPE_BASE = 10000.0


def layer_norm(x_in, scale):
    x_f32 = x_in.astype(jnp.float32)
    centered = x_f32 - jnp.mean(x_f32, axis=-1, keepdims=True)
    variance = jnp.mean(centered * centered, axis=-1, keepdims=True)
    return (centered * lax.rsqrt(variance + LN_EPS) * scale).astype(jnp.bfloat16)


def rope_tables(seq_len, head_dim):
    positions = jnp.arange(seq_len).astype(jnp.float32)
    inv_freq = ROPE_BASE ** (-jnp.arange(0, head_dim, 2).astype(jnp.float32) / head_dim)
    angles = positions[:, None] * inv_freq[None, :]
    return jnp.cos(angles), jnp.sin(angles)


def rotate(x_in, cos_t, sin_t):
    half_dim = x_in.shape[-1] // 2
    x_lo = x_in[..., :half_dim]
    x_hi = x_in[..., half_dim:]
    return jnp.concatenate([x_lo * cos_t - x_hi * sin_t, x_hi * cos_t + x_lo * sin_t], axis=-1)


def adam_update(param_in, grad_in, mom_in, vel_in):
    mom_new = BETA_ONE * mom_in + (1.0 - BETA_ONE) * grad_in
    vel_new = BETA_TWO * vel_in + (1.0 - BETA_TWO) * grad_in * grad_in
    return param_in - LEARN_RATE * mom_new / (jnp.sqrt(vel_new) + ADAM_EPS), mom_new, vel_new


def setup_inputs(seed: int = 0) -> dict:
    keys = jax.random.split(jax.random.key(seed), 24)
    drawn = {}
    drawn['tokens'] = jax.random.randint(keys[0], (BATCH_ALL, SEQ_LEN), 0, VOCAB_SIZE, dtype=jnp.int32)
    drawn['labels'] = jax.random.randint(keys[1], (BATCH_ALL, SEQ_LEN), 0, VOCAB_SIZE, dtype=jnp.int32)
    names = ['embed', 'ln_scales', 'w_q', 'w_kv', 'w_o', 'w_gu', 'w_down']
    params = [
        jax.random.normal(keys[2], (VOCAB_SIZE, D_MODEL), jnp.float32),
        jax.random.uniform(keys[3], (2, D_MODEL), jnp.float32, 0.5, 1.5),
        jax.random.normal(keys[4], (D_MODEL, N_HEADS * HEAD_DIM), jnp.float32) * D_MODEL ** -0.5,
        jax.random.normal(keys[5], (2, D_MODEL, HEAD_DIM), jnp.float32) * D_MODEL ** -0.5,
        jax.random.normal(keys[6], (N_HEADS * HEAD_DIM, D_MODEL), jnp.float32) * (N_HEADS * HEAD_DIM) ** -0.5,
        jax.random.normal(keys[7], (2, D_MODEL, FF_DIM), jnp.float32) * D_MODEL ** -0.5,
        jax.random.normal(keys[8], (FF_DIM, D_MODEL), jnp.float32) * FF_DIM ** -0.5,
    ]
    for index in range(7):
        drawn[names[index]] = params[index]
    grad_scale = (BATCH_ALL * SEQ_LEN * D_MODEL) ** -0.5
    mom_scales = [grad_scale * VOCAB_SIZE ** -0.5, 8.0 / D_MODEL, grad_scale, grad_scale, grad_scale, grad_scale, grad_scale]
    vel_scales = [grad_scale * VOCAB_SIZE ** -0.5, 3.0 / D_MODEL, grad_scale, grad_scale, grad_scale, grad_scale, grad_scale]
    for index in range(7):
        drawn['m_' + names[index]] = mom_scales[index] * jax.random.normal(keys[9 + index], params[index].shape, jnp.float32)
    for index in range(7):
        drawn['v_' + names[index]] = vel_scales[index] * vel_scales[index] * jax.random.uniform(keys[16 + index], params[index].shape, jnp.float32, 0.5, 2.0)
    return drawn


def sequence_loss(param_set, tok_row, lab_row):
    emb_b = param_set[0].astype(jnp.bfloat16)
    ln_scales = param_set[1]
    wq_b = param_set[2].astype(jnp.bfloat16)
    wkv_b = param_set[3].astype(jnp.bfloat16)
    wo_b = param_set[4].astype(jnp.bfloat16)
    wgu_b = param_set[5].astype(jnp.bfloat16)
    wdown_b = param_set[6].astype(jnp.bfloat16)
    x_zero = jnp.take(emb_b, tok_row, axis=0)
    u_norm = layer_norm(x_zero, ln_scales[0])
    q_raw = jnp.dot(u_norm, wq_b, preferred_element_type=jnp.float32).reshape(SEQ_LEN, N_HEADS, HEAD_DIM)
    k_raw = jnp.dot(u_norm, wkv_b[0], preferred_element_type=jnp.float32)
    values = jnp.dot(u_norm, wkv_b[1], preferred_element_type=jnp.float32).astype(jnp.bfloat16)
    cos_t, sin_t = rope_tables(SEQ_LEN, HEAD_DIM)
    queries = rotate(q_raw, cos_t[:, None, :], sin_t[:, None, :]).astype(jnp.bfloat16)
    key_rot = rotate(k_raw, cos_t, sin_t).astype(jnp.bfloat16)
    scores = jnp.einsum('qhe,ke->hqk', queries.astype(jnp.float32), key_rot.astype(jnp.float32)) * HEAD_DIM ** -0.5
    causal = jnp.arange(SEQ_LEN)[:, None] >= jnp.arange(SEQ_LEN)[None, :]
    prob_b16 = jax.nn.softmax(jnp.where(causal, scores, -1e30), axis=-1).astype(jnp.bfloat16)
    context = jnp.einsum('hqk,ke->qhe', prob_b16.astype(jnp.float32), values.astype(jnp.float32)).astype(jnp.bfloat16)
    att_out = jnp.dot(context.reshape(SEQ_LEN, N_HEADS * HEAD_DIM), wo_b, preferred_element_type=jnp.float32)
    gate = jnp.dot(u_norm, wgu_b[0], preferred_element_type=jnp.float32)
    up_val = jnp.dot(u_norm, wgu_b[1], preferred_element_type=jnp.float32)
    hidden = (jax.nn.silu(gate) * up_val).astype(jnp.bfloat16)
    mlp_out = jnp.dot(hidden, wdown_b, preferred_element_type=jnp.float32)
    x_one = x_zero.astype(jnp.float32) + att_out + mlp_out
    f_norm = layer_norm(x_one, ln_scales[1])
    logits = jnp.dot(f_norm, emb_b.T, preferred_element_type=jnp.float32) * D_MODEL ** -0.5
    log_norm = jax.nn.logsumexp(logits, axis=-1)
    lab_logit = jnp.take_along_axis(logits, lab_row[:, None], axis=-1)[:, 0]
    return jnp.sum(log_norm - lab_logit + LOGIT_ZLOSS * log_norm * log_norm)


def reference(tokens, labels, embed, ln_scales, w_q, w_kv, w_o, w_gu, w_down, m_embed, m_ln_scales, m_w_q, m_w_kv, m_w_o, m_w_gu, m_w_down, v_embed, v_ln_scales, v_w_q, v_w_kv, v_w_o, v_w_gu, v_w_down):
    params = (embed, ln_scales, w_q, w_kv, w_o, w_gu, w_down)

    def total_loss(param_set):
        def one_seq(row_pair):
            return sequence_loss(param_set, row_pair[0], row_pair[1])
        per_seq = lax.map(jax.checkpoint(one_seq), (tokens, labels))
        return jnp.sum(per_seq) / (BATCH_ALL * SEQ_LEN)

    loss, gradients = jax.value_and_grad(total_loss)(params)
    new_embed, new_m_embed, new_v_embed = adam_update(embed, gradients[0], m_embed, v_embed)
    new_ln_scales, new_m_ln_scales, new_v_ln_scales = adam_update(ln_scales, gradients[1], m_ln_scales, v_ln_scales)
    new_w_q, new_m_w_q, new_v_w_q = adam_update(w_q, gradients[2], m_w_q, v_w_q)
    new_w_kv, new_m_w_kv, new_v_w_kv = adam_update(w_kv, gradients[3], m_w_kv, v_w_kv)
    new_w_o, new_m_w_o, new_v_w_o = adam_update(w_o, gradients[4], m_w_o, v_w_o)
    new_w_gu, new_m_w_gu, new_v_w_gu = adam_update(w_gu, gradients[5], m_w_gu, v_w_gu)
    new_w_down, new_m_w_down, new_v_w_down = adam_update(w_down, gradients[6], m_w_down, v_w_down)
    return (new_embed, new_ln_scales, new_w_q, new_w_kv, new_w_o, new_w_gu, new_w_down,
            new_m_embed, new_m_ln_scales, new_m_w_q, new_m_w_kv, new_m_w_o, new_m_w_gu, new_m_w_down,
            new_v_embed, new_v_ln_scales, new_v_w_q, new_v_w_kv, new_v_w_o, new_v_w_gu, new_v_w_down,
            loss)
```

```python
import functools
import math

import jax
import jax.numpy as jnp
from jax import lax
from jax.experimental import pallas as pl
from jax.experimental.pallas import tpu as pltpu
from jax.sharding import PartitionSpec as P

LN_EPS = 1e-5
LOGIT_ZLOSS = 1e-4
LEARN_RATE = 1e-2
BETA_ONE = 0.9
BETA_TWO = 0.95
ADAM_EPS = 1e-8
ROPE_BASE = 10000.0
LOG2E = math.log2(math.e)

FWD_TILE = 2048
FWD_CHUNK = 256
ROW_TILE = 512


def norm_fwd(x_in, scale):
    x_f32 = x_in.astype(jnp.float32)
    centered = x_f32 - jnp.mean(x_f32, axis=-1, keepdims=True)
    inv_std = lax.rsqrt(jnp.mean(centered * centered, axis=-1, keepdims=True) + LN_EPS)
    x_hat = centered * inv_std
    return (x_hat * scale).astype(jnp.bfloat16), x_hat, inv_std


def norm_bwd(d_out, x_hat, inv_std, scale):
    d_scale = jnp.sum(d_out * x_hat, axis=(0, 1))
    d_hat = d_out * scale
    d_in = inv_std * (d_hat - jnp.mean(d_hat, axis=-1, keepdims=True) - x_hat * jnp.mean(d_hat * x_hat, axis=-1, keepdims=True))
    return d_in, d_scale


def rope_tables(seq_len, head_dim):
    positions = jnp.arange(seq_len).astype(jnp.float32)
    inv_freq = ROPE_BASE ** (-jnp.arange(0, head_dim, 2).astype(jnp.float32) / head_dim)
    angles = positions[:, None] * inv_freq[None, :]
    return jnp.cos(angles), jnp.sin(angles)


def rotate(x_in, cos_t, sin_t):
    half_dim = x_in.shape[-1] // 2
    x_lo = x_in[..., :half_dim]
    x_hi = x_in[..., half_dim:]
    return jnp.concatenate([x_lo * cos_t - x_hi * sin_t, x_hi * cos_t + x_lo * sin_t], axis=-1)


def adam_update(param_in, grad_in, mom_in, vel_in):
    mom_new = BETA_ONE * mom_in + (1.0 - BETA_ONE) * grad_in
    vel_new = BETA_TWO * vel_in + (1.0 - BETA_TWO) * grad_in * grad_in
    return param_in - LEARN_RATE * mom_new / (jnp.sqrt(vel_new) + ADAM_EPS), mom_new, vel_new


def swap_tp(x):
    return lax.ppermute(x, 'tp', [(0, 1), (1, 0)])


def swap_core(x):
    return lax.ppermute(x, 'dp', [(0, 1), (1, 0), (2, 3), (3, 2)])


def swap_chip(x):
    return lax.ppermute(x, 'dp', [(0, 2), (2, 0), (1, 3), (3, 1)])


def in_order(mine, other, place):
    first = jnp.where(place == 0, mine, other)
    second = jnp.where(place == 0, other, mine)
    return jnp.concatenate([first, second], axis=0)


def gather_dp(x, chip, core):
    pair = in_order(x, swap_core(x), core)
    far = swap_chip(x)
    far_pair = in_order(far, swap_core(far), core)
    return in_order(pair, far_pair, chip)


def sum_dp(x, core, split):
    s = x + swap_core(x)
    if not split:
        return s + swap_chip(s)
    half = x.shape[0] // 2
    mine = lax.dynamic_slice_in_dim(s, core * half, half, axis=0)
    mine = mine + swap_chip(mine)
    return in_order(mine, swap_core(mine), core)


def logit_fwd_kernel(tail, e_ref, ft_ref, acc_out, stat_out, z_scr, acc, m_scr, s_scr):
    step = pl.program_id(0)
    last = pl.num_programs(0) - 1
    width = ft_ref.shape[1]
    k = LOG2E * e_ref.shape[1] ** -0.5

    @pl.when(step == 0)
    def _():
        acc[...] = jnp.zeros_like(acc)
        m_scr[...] = jnp.full_like(m_scr, -1e38)
        s_scr[...] = jnp.zeros_like(s_scr)

    def tile(rows):
        chunks = [(lo, min(FWD_CHUNK, rows - lo)) for lo in range(0, rows, FWD_CHUNK)]
        top = m_scr[...]
        for lo, n in chunks:
            e_b = e_ref[lo:lo + n, :].astype(jnp.bfloat16)
            z = jnp.dot(e_b, ft_ref[...], preferred_element_type=jnp.float32)
            z_scr[lo:lo + n, :] = z
            top = jnp.maximum(top, jnp.max(z.reshape(n // 8, 8, width), axis=0))
        m_new = jnp.max(top, axis=0, keepdims=True)
        alpha = jnp.exp2((m_scr[0:1, :] - m_new) * k)
        m_scr[...] = jnp.broadcast_to(m_new, m_scr.shape)
        sums = s_scr[...] * alpha
        acc[...] = acc[...] * alpha
        for lo, n in chunks:
            p = jnp.exp2((z_scr[lo:lo + n, :] - m_new) * k)
            sums = sums + jnp.sum(p.reshape(n // 8, 8, width), axis=0)
            e_t = e_ref[lo:lo + n, :].T.astype(jnp.bfloat16)
            acc[...] += jnp.dot(e_t, p.astype(jnp.bfloat16), preferred_element_type=jnp.float32)
        s_scr[...] = sums

    @pl.when(step < last)
    def _():
        tile(FWD_TILE)

    @pl.when(step == last)
    def _():
        tile(tail)
        acc_out[...] = acc[...].T
        row = lax.broadcasted_iota(jnp.int32, stat_out.shape, 0)
        total = jnp.sum(s_scr[...], axis=0, keepdims=True)
        stat_out[...] = jnp.where(row == 0, m_scr[...], jnp.broadcast_to(total, stat_out.shape))


def logit_fwd(embed, f_t):
    vocab, d_model = embed.shape
    width = f_t.shape[1]
    steps = pl.cdiv(vocab, FWD_TILE)
    tail = vocab - (steps - 1) * FWD_TILE
    return pl.pallas_call(
        functools.partial(logit_fwd_kernel, tail),
        grid=(steps,),
        out_shape=(jax.ShapeDtypeStruct((width, d_model), jnp.float32), jax.ShapeDtypeStruct((8, width), jnp.float32)),
        in_specs=[pl.BlockSpec((FWD_TILE, d_model), lambda i: (i, 0)), pl.BlockSpec((d_model, width), lambda i: (0, 0))],
        out_specs=(pl.BlockSpec((width, d_model), lambda i: (0, 0)), pl.BlockSpec((8, width), lambda i: (0, 0))),
        scratch_shapes=[pltpu.VMEM((FWD_TILE, width), jnp.float32), pltpu.VMEM((d_model, width), jnp.float32),
                        pltpu.VMEM((8, width), jnp.float32), pltpu.VMEM((8, width), jnp.float32)],
        compiler_params=pltpu.CompilerParams(dimension_semantics=("arbitrary",), vmem_limit_bytes=48 << 20),
        cost_estimate=pl.CostEstimate(flops=4 * vocab * width * d_model, bytes_accessed=vocab * d_model * 4, transcendentals=vocab * width),
        name="logit_fwd",
    )(embed, f_t)


def head_grad_kernel(chunk, base_ref, e_ref, f_ref, ft_ref, c_ref, *rest):
    out_ref = rest[-1]
    k = LOG2E * e_ref.shape[1] ** -0.5
    e_b = e_ref[...].astype(jnp.bfloat16)
    total = None
    for lo in range(0, f_ref.shape[0], chunk):
        z = jnp.dot(e_b, ft_ref[:, lo:lo + chunk], preferred_element_type=jnp.float32)
        p = jnp.exp2(z * k - c_ref[0:1, lo:lo + chunk]) * c_ref[1:2, lo:lo + chunk]
        part = jnp.dot(p.astype(jnp.bfloat16), f_ref[lo:lo + chunk, :], preferred_element_type=jnp.float32)
        total = part if total is None else total + part
    out_ref[...] = total


def head_grad(base, first, count, all_blocks, embed, f_all, f_all_t, coefs, grad):
    d_model = embed.shape[1]
    tokens = f_all.shape[0]
    args = [base, embed, f_all, f_all_t, coefs]
    in_specs = [pl.BlockSpec((ROW_TILE, d_model), lambda i, b: (b[0] + first + i, 0)),
                pl.BlockSpec((tokens, d_model), lambda i, b: (0, 0)),
                pl.BlockSpec((d_model, tokens), lambda i, b: (0, 0)),
                pl.BlockSpec((8, tokens), lambda i, b: (0, 0))]
    aliases = {}
    if grad is not None:
        args.append(grad)
        in_specs.append(pl.BlockSpec(memory_space=pl.ANY))
        aliases = {5: 0}
    return pl.pallas_call(
        functools.partial(head_grad_kernel, 512),
        grid_spec=pltpu.PrefetchScalarGridSpec(
            num_scalar_prefetch=1, grid=(count,), in_specs=in_specs,
            out_specs=pl.BlockSpec((ROW_TILE, d_model), lambda i, b: (first + i, 0))),
        out_shape=jax.ShapeDtypeStruct((all_blocks * ROW_TILE, d_model), jnp.float32),
        input_output_aliases=aliases,
        compiler_params=pltpu.CompilerParams(dimension_semantics=("arbitrary",), vmem_limit_bytes=48 << 20),
        cost_estimate=pl.CostEstimate(flops=4 * count * ROW_TILE * tokens * d_model, bytes_accessed=count * ROW_TILE * d_model * 8,
                                      transcendentals=count * ROW_TILE * tokens),
        name="head_grad_" + str(first),
    )(*args)


def table_adam_kernel(base_ref, starts_ref, order_ref, ids_ref, p_ref, m_ref, v_ref, g_ref, rows_ref, *rest):
    po_ref, mo_ref, vo_ref, g_scr = rest[-4:]
    block = base_ref[0] + pl.program_id(0)
    g_scr[...] = g_ref[...]
    low = block * ROW_TILE

    def add_row(i, carry):
        src = order_ref[i]
        dst = ids_ref[i] - low
        g_scr[pl.ds(dst, 1), :] += rows_ref[pl.ds(src, 1), :]
        return carry

    lax.fori_loop(starts_ref[block], starts_ref[block + 1], add_row, 0)
    po_ref[...], mo_ref[...], vo_ref[...] = adam_update(p_ref[...], g_scr[...], m_ref[...], v_ref[...])


def table_adam(base, count, starts, order, ids, state, grad, rows, prior):
    vocab, d_model = state[0].shape
    at = pl.BlockSpec((ROW_TILE, d_model), lambda i, b, *_: (b[0] + i, 0))
    in_specs = [at, at, at, pl.BlockSpec((ROW_TILE, d_model), lambda i, *_: (i, 0)),
                pl.BlockSpec(rows.shape, lambda i, *_: (0, 0), pipeline_mode=pl.Buffered(1))]
    args = [base, starts, order, ids] + list(state) + [grad, rows]
    aliases = {}
    if prior is not None:
        in_specs += [pl.BlockSpec(memory_space=pl.ANY)] * 3
        args += list(prior)
        aliases = {9: 0, 10: 1, 11: 2}
    return pl.pallas_call(
        table_adam_kernel,
        grid_spec=pltpu.PrefetchScalarGridSpec(
            num_scalar_prefetch=4, grid=(count,), in_specs=in_specs, out_specs=(at, at, at),
            scratch_shapes=[pltpu.VMEM((ROW_TILE, d_model), jnp.float32)]),
        out_shape=tuple(jax.ShapeDtypeStruct((vocab, d_model), jnp.float32) for _ in range(3)),
        input_output_aliases=aliases,
        compiler_params=pltpu.CompilerParams(dimension_semantics=("arbitrary",), vmem_limit_bytes=48 << 20),
        cost_estimate=pl.CostEstimate(flops=20 * 1000 * count * ROW_TILE * d_model, bytes_accessed=count * ROW_TILE * d_model * 28, transcendentals=0),
        name="table_adam",
    )(*args)


def solution(mesh):
    dp_size = mesh.shape['dp']
    param_specs = (P('tp', None), P(None, None), P(None, 'tp'), P(None, None, None), P('tp', None), P(None, None, 'tp'), P('tp', None))

    def local_step(tokens, labels, *state_arrays):
        embed, ln_scales, w_q, w_kv, w_o, w_gu, w_down = state_arrays[0:7]
        batch_loc, seq_len = tokens.shape
        vocab_loc, d_model = embed.shape
        head_dim = w_kv.shape[2]
        heads_loc = w_q.shape[1] // head_dim
        tok_total = batch_loc * seq_len * dp_size
        tp_rank = lax.axis_index('tp')
        dp_rank = lax.axis_index('dp')
        chip, core = dp_rank // 2, dp_rank % 2
        wq_b = w_q.astype(jnp.bfloat16)
        wkv_b = w_kv.astype(jnp.bfloat16)
        wo_b = w_o.astype(jnp.bfloat16).reshape(heads_loc, head_dim, d_model)
        wgu_b = w_gu.astype(jnp.bfloat16)
        wdown_b = w_down.astype(jnp.bfloat16)

        def local_rows(ids):
            loc = ids - tp_rank * vocab_loc
            ok = (loc >= 0) & (loc < vocab_loc)
            got = embed.at[jnp.where(ok, loc, 0)].get(mode="promise_in_bounds").astype(jnp.bfloat16).astype(jnp.float32)
            return jnp.where(ok[..., None], got, 0.0)

        x_part = local_rows(tokens)
        x_zero = x_part + swap_tp(x_part)
        lab_rows = local_rows(labels)

        both = jnp.concatenate([tokens, labels], axis=0)[None]
        both_all = gather_dp(both, chip, core)
        ids_all = jnp.concatenate([both_all[:, 0].reshape(-1), both_all[:, 1].reshape(-1)]) - tp_rank * vocab_loc
        ids_sorted, order = lax.sort((ids_all, jnp.arange(2 * tok_total, dtype=jnp.int32)), num_keys=1, is_stable=False)
        blocks = pl.cdiv(vocab_loc, ROW_TILE)
        blocks += blocks % 2
        edges = jnp.minimum(jnp.arange(blocks + 1, dtype=jnp.int32) * ROW_TILE, vocab_loc)
        starts = jnp.sum((ids_all[None, :] < edges[:, None]).astype(jnp.int32), axis=1)

        u_norm, u_hat, u_inv = norm_fwd(x_zero, ln_scales[0])
        cos_t, sin_t = rope_tables(seq_len, head_dim)
        q_raw = jnp.einsum('bsd,dn->bsn', u_norm, wq_b, preferred_element_type=jnp.float32).reshape(batch_loc, seq_len, heads_loc, head_dim)
        queries = rotate(q_raw, cos_t[:, None, :], sin_t[:, None, :]).astype(jnp.bfloat16)
        kv_raw = jnp.einsum('bsd,cde->cbse', u_norm, wkv_b, preferred_element_type=jnp.float32)
        key_rot = rotate(kv_raw[0], cos_t, sin_t).astype(jnp.bfloat16)
        values = kv_raw[1].astype(jnp.bfloat16)
        causal = jnp.arange(seq_len)[:, None] >= jnp.arange(seq_len)[None, :]
        scores = jnp.einsum('bqhe,bke->bhqk', queries, key_rot, preferred_element_type=jnp.float32) * head_dim ** -0.5
        prob_f32 = jax.nn.softmax(jnp.where(causal, scores, -1e30), axis=-1)
        prob_b16 = prob_f32.astype(jnp.bfloat16)
        context = jnp.einsum('bhqk,bke->bqhe', prob_b16, values, preferred_element_type=jnp.float32).astype(jnp.bfloat16)
        att_part = jnp.einsum('crif,ife->cre', context, wo_b, preferred_element_type=jnp.float32)
        gate_up = jnp.einsum('bsd,cdf->cbsf', u_norm, wgu_b, preferred_element_type=jnp.float32)
        gate_sig = jax.nn.sigmoid(gate_up[0])
        hidden = (gate_up[0] * gate_sig * gate_up[1]).astype(jnp.bfloat16)
        mlp_part = jnp.einsum('bsf,fd->bsd', hidden, wdown_b, preferred_element_type=jnp.float32)
        block_part = att_part + mlp_part
        x_one = x_zero + (block_part + swap_tp(block_part))
        f_norm, f_hat, f_inv = norm_fwd(x_one, ln_scales[1])

        grad_scale = d_model ** -0.5 / tok_total
        f_two = f_norm.reshape(seq_len, d_model)
        f_wide = f_two.astype(jnp.float32)
        f_all_wide = lax.optimization_barrier(gather_dp(f_wide, chip, core))
        f_all = f_all_wide.astype(jnp.bfloat16)
        f_all_t = f_all.T
        acc, stats = logit_fwd(embed, f_two.T)
        lab_part = jnp.sum(f_wide * lab_rows.reshape(seq_len, d_model), axis=-1)
        my_stats = jnp.concatenate([stats[0:2], lab_part[None, :], jnp.zeros((5, seq_len), jnp.float32)], axis=0)
        its_stats = swap_tp(my_stats)
        row_max = jnp.maximum(my_stats[0], its_stats[0])
        my_weight = jnp.exp2((my_stats[0] - row_max) * (LOG2E * d_model ** -0.5))
        its_weight = jnp.exp2((its_stats[0] - row_max) * (LOG2E * d_model ** -0.5))
        sum_exp = my_stats[1] * my_weight + its_stats[1] * its_weight
        log_norm = row_max * d_model ** -0.5 + jnp.log(sum_exp)
        lab_logit = (my_stats[2] + its_stats[2]) * d_model ** -0.5
        tok_loss = log_norm - lab_logit + LOGIT_ZLOSS * log_norm * log_norm
        z_factor = 1.0 + 2.0 * LOGIT_ZLOSS * log_norm
        sent = jnp.concatenate([log_norm[None], tok_loss[None], jnp.zeros((6, seq_len), jnp.float32)], axis=0)[None]
        got = gather_dp(sent, chip, core)
        log_all = got[:, 0].reshape(-1)
        loss = jnp.sum(got[:, 1]) / tok_total
        coefs = jnp.concatenate([(log_all * LOG2E)[None], ((1.0 + 2.0 * LOGIT_ZLOSS * log_all) * grad_scale)[None],
                                 jnp.zeros((6, tok_total), jnp.float32)], axis=0)

        d_fin_part = acc * (z_factor / sum_exp * my_weight * grad_scale)[:, None] - lab_rows.reshape(seq_len, d_model) * grad_scale
        d_fin = (d_fin_part + swap_tp(d_fin_part)).reshape(batch_loc, seq_len, d_model)

        half_blocks = blocks // 2
        base = (core * half_blocks).astype(jnp.int32)[None]
        other_base = ((1 - core) * half_blocks).astype(jnp.int32)[None]
        cut_a, cut_b = (half_blocks * 9) // 25, (half_blocks * 17) // 25
        grad_a = head_grad(base, 0, cut_a, half_blocks, embed, f_all, f_all_t, coefs, None)
        grad_a, d_fin = lax.optimization_barrier((grad_a, d_fin))

        d_one, g_ln_fin = norm_bwd(d_fin, f_hat, f_inv, ln_scales[1])
        d_one_b = d_one.astype(jnp.bfloat16)

        d_hidden = jnp.einsum('bsd,fd->bsf', d_one_b, wdown_b, preferred_element_type=jnp.float32)
        g_down = jnp.einsum('bsf,bsd->fd', hidden, d_one_b, preferred_element_type=jnp.float32)
        d_gate = d_hidden * gate_up[1] * gate_sig * (1.0 + gate_up[0] * (1.0 - gate_sig))
        d_up = d_hidden * gate_up[0] * gate_sig
        d_gate_up = jnp.stack([d_gate, d_up]).astype(jnp.bfloat16)
        g_gu = jnp.einsum('cbsf,bsd->cdf', d_gate_up, u_norm, preferred_element_type=jnp.float32)
        d_u_mlp = jnp.einsum('cbsf,cdf->bsd', d_gate_up, wgu_b, preferred_element_type=jnp.float32)

        d_context = jnp.einsum('cre,ife->crif', d_one_b, wo_b, preferred_element_type=jnp.float32).astype(jnp.bfloat16)
        g_o = jnp.einsum('crif,cre->ife', context, d_one_b, preferred_element_type=jnp.float32).reshape(heads_loc * head_dim, d_model)
        d_probs = jnp.einsum('bqhe,bke->bhqk', d_context, values, preferred_element_type=jnp.float32)
        d_values = jnp.einsum('bhqk,bqhe->bke', prob_b16, d_context, preferred_element_type=jnp.float32)
        d_scores = (prob_f32 * (d_probs - jnp.sum(d_probs * prob_f32, axis=-1, keepdims=True)) * head_dim ** -0.5).astype(jnp.bfloat16)
        d_queries = jnp.einsum('bhqk,bke->bqhe', d_scores, key_rot, preferred_element_type=jnp.float32)
        d_keys = jnp.einsum('bhqk,bqhe->bke', d_scores, queries, preferred_element_type=jnp.float32)
        d_q_raw = rotate(d_queries, cos_t[:, None, :], -sin_t[:, None, :]).astype(jnp.bfloat16).reshape(batch_loc, seq_len, heads_loc * head_dim)
        d_kv = jnp.stack([rotate(d_keys, cos_t, -sin_t), d_values]).astype(jnp.bfloat16)
        g_q = jnp.einsum('bsd,bsn->dn', u_norm, d_q_raw, preferred_element_type=jnp.float32)
        g_kv_part = jnp.einsum('cbse,bsd->cde', d_kv, u_norm, preferred_element_type=jnp.float32)
        d_u_att = (jnp.einsum('bsn,dn->bsd', d_q_raw, wq_b, preferred_element_type=jnp.float32)
                   + jnp.einsum('cbse,cde->bsd', d_kv, wkv_b, preferred_element_type=jnp.float32))
        d_u_part = d_u_att + d_u_mlp
        d_u = d_u_part + swap_tp(d_u_part)

        grad_a, _ = lax.optimization_barrier((grad_a, d_u_part))
        grad_b = head_grad(base, cut_a, cut_b - cut_a, half_blocks, embed, f_all, f_all_t, coefs, grad_a)
        grad_b, d_u = lax.optimization_barrier((grad_b, d_u))
        d_zero_norm, g_ln_in = norm_bwd(d_u, u_hat, u_inv, ln_scales[0])
        d_zero = (d_one + d_zero_norm).reshape(seq_len, d_model)
        grad_b, d_zero = lax.optimization_barrier((grad_b, d_zero))
        rows = jnp.concatenate([gather_dp(d_zero, chip, core), f_all_wide * -grad_scale], axis=0)
        grad_c = head_grad(base, cut_b, half_blocks - cut_b, half_blocks, embed, f_all, f_all_t, coefs, grad_b)
        grad_other = swap_core(grad_c)

        g_kv = g_kv_part + swap_tp(g_kv_part)
        g_ln = jnp.stack([g_ln_in, g_ln_fin])
        gradients = (None, sum_dp(g_ln, core, False), sum_dp(g_q, core, False), sum_dp(g_kv, core, False), sum_dp(g_o, core, False),
                     sum_dp(g_gu, core, True), sum_dp(g_down, core, True))

        table = (embed, state_arrays[7], state_arrays[14])
        mine = table_adam(base, half_blocks, starts, order, ids_sorted, table, grad_c, rows, None)
        news = [table_adam(other_base, half_blocks, starts, order, ids_sorted, table, grad_other, rows, mine)]
        for index in range(1, 7):
            news.append(adam_update(state_arrays[index], gradients[index], state_arrays[7 + index], state_arrays[14 + index]))
        return tuple(n[0] for n in news) + tuple(n[1] for n in news) + tuple(n[2] for n in news) + (loss,)

    return jax.shard_map(local_step, mesh=mesh, in_specs=(P('dp', None), P('dp', None)) + param_specs * 3,
                         out_specs=param_specs * 3 + (P(),), check_vma=False)
```
